32 devices in a mesh: groups: 2 (over x), expert: 16 (over z, y, core).
Axes of the slice: x: 2, y: 2, z: 4, core: 2. Of those that a mesh axis runs over, the one named last changes fastest.
Arguments:
- query_features: bfloat16 [4096, 1024], P(('groups', 'expert')), parts along dimension 0, may hold values from -6 to 6
- query_job_label: int32 [4096], P(('groups', 'expert')), parts along dimension 0, may hold values from 0 to 7, as said below
- selected_specialists: int32 [4096, 2], P(('groups', 'expert')), parts along dimension 0, may hold values from 0 to 8, as said below
- whole_number_mixing_factors: int32 [4096, 2], P(('groups', 'expert')), parts along dimension 0, may hold values from 1 to 8
- copy_room_sizes: int32 [16], replicated, may hold values from 256 to 384, as said below
- first_layer_matrix: bfloat16 [16, 1024, 2048], P('expert'), as said below
- second_layer_matrix: bfloat16 [16, 2048, 1024], P('expert'), as said below
Outputs:
- mixture: bfloat16 [4096, 1024], P(('groups', 'expert')), parts along dimension 0
The draws below stay inside these ranges and needn't reach their ends.
There are 2 independent parts, one for each index of `groups`. The reference program is written for one: setup_inputs(seed, part) draws one part's arguments, and reference() takes and returns one part's arrays. A program takes and returns all parts, laid end to end along the dimension named above; an argument that names none is the same for every part. Nothing has to cross between parts.
Inputs may be any that keep to these rules, and one draw needn't show every extreme that they name: `query_job_label`: each request's task number; column 0 of `selected_specialists` names a task expert of this task. `selected_specialists`: column 0 names a task expert of the row's task (number r from 8 on is task expert r - 8), column 1 a shared expert (below 8). From the rows of one device at most 32 entries go to one expert copy, and in every draw some copy receives exactly 32 entries from every device. `copy_room_sizes`: some copy has capacity 384 and some copy 2 * 128. `first_layer_matrix`: the 1 copies of one shared expert hold equal weights. `second_layer_matrix`: the 1 copies of one shared expert hold equal weights.
All inputs are finite; a program needn't handle non-finite values.
Results may differ from the reference program's by a relative error of at most 0.0058.
Values may be sent and summed in bfloat16 or wider, within the bound.
No kernel may reach another device: no remote copies, remote signals or barrier semaphores. Data moves between devices by JAX's collectives and lax.ppermute only.
A program may use at most 64 MiB of HBM per device.

```python
import jax
import jax.numpy as jnp
from jax import lax

D = 1024
HIDDEN_SIZE = 2048
TASKS = 8
SHARED = 8
TOP = 2
ROWS_DEV = 128
EXPERTS = 16
REPL = 1
TASK_EXP = 1
SLOT = 32
CAPACITY = 384
ROWS = 2048


def pick_tickets(device_key, popular, hottest, wanted, slots):
    tickets = popular.shape[0] * slots
    owners = jnp.arange(tickets, dtype=jnp.int32) // slots
    jitter = jax.random.randint(jax.random.fold_in(device_key, 1), (tickets,), 0, 16384)
    scores = jitter + popular[owners] + jnp.where(owners == hottest, 1 << 20, 0)
    ranking = jnp.argsort(-scores, stable=True)
    chosen = owners[ranking[:wanted]]
    shuffled = jax.random.permutation(jax.random.fold_in(device_key, 2), wanted)
    return chosen[shuffled]


def routing_plan(key):
    base_key = jax.random.fold_in(key, 11)
    task_copies = TASKS * TASK_EXP
    group_rows = ROWS_DEV // REPL
    task_popular = jax.random.randint(jax.random.fold_in(base_key, 1), (task_copies,), 0, 8192)
    task_hottest = jax.random.randint(jax.random.fold_in(base_key, 2), (), 0, task_copies)
    shared_popular = jax.random.randint(jax.random.fold_in(base_key, 3), (SHARED,), 0, 8192)
    shared_hottest = jax.random.randint(jax.random.fold_in(base_key, 4), (), 0, SHARED)
    task_base = jax.random.fold_in(base_key, 5)
    shared_base = jax.random.fold_in(base_key, 6)

    def task_device(device):
        return pick_tickets(jax.random.fold_in(task_base, device), task_popular, task_hottest, ROWS_DEV, SLOT)

    def shared_group(group):
        return pick_tickets(jax.random.fold_in(shared_base, group), shared_popular, shared_hottest, group_rows, SLOT)
    task_choice = jax.vmap(task_device)(jnp.arange(EXPERTS, dtype=jnp.int32)).reshape(ROWS)
    shared_choice = jax.vmap(shared_group)(jnp.arange(EXPERTS * REPL, dtype=jnp.int32))
    shared_flat = shared_choice.reshape(EXPERTS, REPL, group_rows).transpose(0, 2, 1).reshape(ROWS)
    tasks = (task_choice // TASK_EXP).astype(jnp.int32)
    numbers = SHARED + task_choice % TASK_EXP
    routing = jnp.stack([numbers, shared_flat], axis=1).astype(jnp.int32)
    return (tasks, routing)


def draw_query_job_label(key, part):
    return routing_plan(key)[0]


def draw_selected_specialists(key, part):
    return routing_plan(key)[1]


def draw_copy_room_sizes(key, part):
    values = jax.random.randint(jax.random.fold_in(key, 1), (EXPERTS,), 2 * ROWS_DEV, CAPACITY + 1)
    top_at = jax.random.randint(jax.random.fold_in(key, 2), (), 0, EXPERTS)
    low_at = (top_at + jax.random.randint(jax.random.fold_in(key, 3), (), 1, EXPERTS)) % EXPERTS
    indices = jnp.arange(EXPERTS, dtype=jnp.int32)
    values = jnp.where(indices == top_at, CAPACITY, values)
    values = jnp.where(indices == low_at, 2 * ROWS_DEV, values)
    return values.astype(jnp.int32)


def copied_weights(key, rows_in, cols_out):
    task_copies = TASKS * TASK_EXP
    shared_part = jax.random.normal(jax.random.fold_in(key, 1), (SHARED, rows_in, cols_out), jnp.float32)
    task_part = jax.random.normal(jax.random.fold_in(key, 2), (task_copies, rows_in, cols_out), jnp.float32)
    stacked = jnp.concatenate([jnp.repeat(shared_part, REPL, axis=0), task_part], axis=0)
    return (stacked * rows_in ** (-0.5)).astype(jnp.bfloat16)


def draw_first_layer_matrix(key, part):
    return copied_weights(jax.random.fold_in(key, 21), D, HIDDEN_SIZE)


def draw_second_layer_matrix(key, part):
    return copied_weights(jax.random.fold_in(key, 22), HIDDEN_SIZE, D)


def place_ends(array, key, least, top_value):
    longest = array.shape.index(max(array.shape))
    spots = []
    for shift in (0, 1):
        where = [jax.random.randint(jax.random.fold_in(key, axis), (), 0, length) for axis, length in enumerate(array.shape)]
        where[longest] = (where[longest] + shift) % array.shape[longest]
        spots.append(tuple(where))
    return array.at[spots[0]].set(least).at[spots[1]].set(top_value)


def block_scale(stream_key, extent, split, smallest, largest):
    def one(position, shards_of):
        draws = jax.random.uniform(jax.random.fold_in(jax.random.fold_in(stream_key, 6), position), (shards_of,), jnp.float32, smallest / len(split), largest / len(split))
        return jnp.repeat(jnp.exp(draws), extent[position] // shards_of).reshape((-1,) + (1,) * (len(extent) - position - 1))

    loudness = one(*split[0])
    for cut in split[1:]:
        loudness = loudness * one(*cut)
    return loudness


def noise(stream_key, shape, deviation, limit, split=(), kind=jnp.bfloat16):
    array = deviation * jax.random.normal(stream_key, shape, jnp.float32)
    if split:
        array = array * block_scale(stream_key, shape, split, -0.22, 0.18)
    return jnp.clip(array, -limit, limit).astype(kind)


def setup_inputs(seed: int = 0, part: int = 0) -> dict:
    splits = jax.random.split(jax.random.key(seed), 8)
    part_splits = jax.random.split(jax.random.fold_in(splits[7], part), 8)
    return {
        "query_features": noise(part_splits[0], (ROWS, D), 1.0, 6.0, ((0, 16),)),
        "query_job_label": draw_query_job_label(jax.random.fold_in(jax.random.fold_in(splits[7], part), 71), part),
        "selected_specialists": draw_selected_specialists(jax.random.fold_in(jax.random.fold_in(splits[7], part), 71), part),
        "whole_number_mixing_factors": place_ends(jax.random.randint(part_splits[3], (ROWS, TOP), 1, 9), jax.random.fold_in(part_splits[3], 1), 1, 8).astype(jnp.int32),
        "copy_room_sizes": draw_copy_room_sizes(jax.random.fold_in(splits[7], 71), part),
        "first_layer_matrix": draw_first_layer_matrix(jax.random.fold_in(splits[7], 71), part),
        "second_layer_matrix": draw_second_layer_matrix(jax.random.fold_in(splits[7], 71), part),
    }


def expert_mlp(block_rows, up_matrix, down_matrix):
    hidden = jax.nn.gelu(jnp.dot(block_rows, up_matrix, preferred_element_type=jnp.float32)).astype(jnp.bfloat16)
    return jnp.dot(hidden, down_matrix, preferred_element_type=jnp.float32).astype(jnp.bfloat16)


def reference(query_features, query_job_label, selected_specialists, whole_number_mixing_factors, copy_room_sizes, first_layer_matrix, second_layer_matrix):
    row_index = jnp.arange(ROWS, dtype=jnp.int32)
    shared_copy = selected_specialists * REPL + (row_index % REPL)[:, None]
    task_copy = SHARED * REPL + query_job_label[:, None] * TASK_EXP + selected_specialists - SHARED
    expert_ids = jnp.where(selected_specialists < SHARED, shared_copy, task_copy).astype(jnp.int32)
    linear_specialist_number = expert_ids.reshape(-1)
    specialist_onehot = (linear_specialist_number[:, None] == jnp.arange(EXPERTS, dtype=jnp.int32)[None, :]).astype(jnp.int32)
    before = jnp.cumsum(specialist_onehot, axis=0) - specialist_onehot
    arrival_rank = jnp.sum(before * specialist_onehot, axis=1).astype(jnp.int32)
    surviving_slot_flags = arrival_rank < copy_room_sizes[linear_specialist_number]
    row_of_entry = (jnp.arange(linear_specialist_number.shape[0], dtype=jnp.int32) // TOP).astype(jnp.int32)

    def one_expert(expert_index):
        target = jnp.where((linear_specialist_number == expert_index) & surviving_slot_flags, arrival_rank, CAPACITY).astype(jnp.int32)
        source = jnp.zeros((CAPACITY,), jnp.int32).at[target].set(row_of_entry, mode="drop")
        live_mask = jnp.zeros((CAPACITY,), jnp.bool_).at[target].set(True, mode="drop")
        block_rows = jnp.where(live_mask[:, None], query_features[source], jnp.zeros((), jnp.bfloat16))
        return expert_mlp(block_rows, first_layer_matrix[expert_index], second_layer_matrix[expert_index])

    outputs = lax.map(one_expert, jnp.arange(EXPERTS, dtype=jnp.int32))
    picked = outputs[linear_specialist_number, jnp.minimum(arrival_rank, CAPACITY - 1)]
    gate_float = whole_number_mixing_factors.astype(jnp.float32)
    gate_share = gate_float / jnp.sum(gate_float, axis=1, keepdims=True)
    row_weight = gate_share.reshape(-1) * surviving_slot_flags.astype(jnp.float32)
    weighted = row_weight[:, None] * picked.astype(jnp.float32)
    return jnp.sum(weighted.reshape(ROWS, TOP, D), axis=1).astype(jnp.bfloat16)
```

```python
import jax
import jax.numpy as jnp
from jax import lax
from jax.sharding import PartitionSpec as P

SHARED = 8


def expert_mlp(block_rows, up_matrix, down_matrix):
    hidden = jax.nn.gelu(jnp.dot(block_rows, up_matrix, preferred_element_type=jnp.float32)).astype(
        jnp.bfloat16
    )
    return jnp.dot(hidden, down_matrix, preferred_element_type=jnp.float32)


def slots_of(ids, slot_size):
    count = ids.shape[0]
    row = lax.broadcasted_iota(jnp.int32, (count, count), 0)
    col = lax.broadcasted_iota(jnp.int32, (count, count), 1)
    before = (ids[:, None] == ids[None, :]) & (col < row)
    return ids * slot_size + jnp.sum(before.astype(jnp.int32), axis=1)


def counts_of(ids, half):
    experts = lax.broadcasted_iota(jnp.int32, (half, ids.shape[0]), 0)
    return jnp.sum((experts == ids[None, :]).astype(jnp.int32), axis=1)


def spread(rows, slots, slot_total):
    place = lax.broadcasted_iota(jnp.int32, (slot_total, rows.shape[0]), 0) == slots[None, :]
    return jnp.dot(place.astype(jnp.bfloat16), rows, preferred_element_type=jnp.float32).astype(
        jnp.bfloat16
    )


def pick(slot_rows, slots):
    place = (
        lax.broadcasted_iota(jnp.int32, (slots.shape[0], slot_rows.shape[0]), 1) == slots[:, None]
    )
    return jnp.dot(place.astype(jnp.bfloat16), slot_rows, preferred_element_type=jnp.float32)


def shards(
    query_features,
    query_job_label,
    selected_specialists,
    whole_number_mixing_factors,
    copy_room_sizes,
    first_layer_matrix,
    second_layer_matrix,
):
    experts = copy_room_sizes.shape[0]
    half = experts // 2
    row_count, width = query_features.shape
    copies = half // SHARED
    slot_size = 4 * row_count // experts
    slot_total = half * slot_size
    up_matrix = first_layer_matrix[0]
    down_matrix = second_layer_matrix[0]
    me = lax.axis_index("expert")
    upper = me >= half
    swap = [(i, (i + half) % experts) for i in range(experts)]
    halves = [list(range(half)), list(range(half, experts))]

    def exchange(array):
        return lax.all_to_all(
            array, "expert", split_axis=0, concat_axis=0, axis_index_groups=halves, tiled=True
        )

    task_id = query_job_label * copies + selected_specialists[:, 0] - SHARED
    row_local = jnp.arange(row_count, dtype=jnp.int32)
    shared_id = selected_specialists[:, 1] * copies + row_local % copies
    near_id = jnp.where(upper, task_id, shared_id)
    far_id = jnp.where(upper, shared_id, task_id)

    guest_rows = lax.ppermute(query_features, "expert", swap)
    guest_id = lax.ppermute(far_id, "expert", swap)

    near_slots = slots_of(near_id, slot_size)
    near_in = exchange(
        spread(query_features, near_slots, slot_total).reshape(half, slot_size, width)
    )
    guest_slots = slots_of(guest_id, slot_size)
    counts = exchange(
        jnp.stack([counts_of(near_id, half), counts_of(guest_id, half)], axis=1)
    )
    guest_in = exchange(spread(guest_rows, guest_slots, slot_total).reshape(half, slot_size, width))

    earlier = (
        lax.broadcasted_iota(jnp.int32, (half, half), 1)
        < lax.broadcasted_iota(jnp.int32, (half, half), 0)
    ).astype(jnp.int32)
    near_base = jnp.sum(earlier * counts[None, :, 0], axis=1) + jnp.where(
        upper, jnp.sum(counts[:, 1]), 0
    )
    guest_base = jnp.sum(earlier * counts[None, :, 1], axis=1) + jnp.where(
        upper, 0, jnp.sum(counts[:, 0])
    )
    room = copy_room_sizes[me]
    slot_local = jnp.arange(slot_size, dtype=jnp.int32)

    def serve(arrived, base):
        keep = (base[:, None] + slot_local[None, :] < room).reshape(-1, 1)
        result = expert_mlp(arrived.reshape(slot_total, width), up_matrix, down_matrix)
        kept = jnp.where(keep, result, 0.0).astype(jnp.bfloat16)
        return exchange(kept.reshape(half, slot_size, width)).reshape(slot_total, width)

    guest_out = pick(serve(guest_in, guest_base), guest_slots).astype(jnp.bfloat16)
    far_out = lax.ppermute(guest_out, "expert", swap).astype(jnp.float32)
    near_out = pick(serve(near_in, near_base), near_slots)

    gate_float = whole_number_mixing_factors.astype(jnp.float32)
    gate_share = gate_float / jnp.sum(gate_float, axis=1, keepdims=True)
    near_share = jnp.where(upper, gate_share[:, 0], gate_share[:, 1])
    far_share = jnp.where(upper, gate_share[:, 1], gate_share[:, 0])
    return (near_share[:, None] * near_out + far_share[:, None] * far_out).astype(jnp.bfloat16)


def solution(mesh):
    in_specs = (
        P(("groups", "expert"), None),
        P(("groups", "expert")),
        P(("groups", "expert"), None),
        P(("groups", "expert"), None),
        P(),
        P("expert", None, None),
        P("expert", None, None),
    )
    out_specs = P(("groups", "expert"), None)
    return jax.shard_map(shards, mesh=mesh, in_specs=in_specs, out_specs=out_specs, check_vma=False)
```

```python
import jax
import jax.numpy as jnp
from jax import lax
from jax.sharding import PartitionSpec as P

SHARED = 8


def expert_mlp(block_rows, up_matrix, down_matrix):
    hidden = jax.nn.gelu(jnp.dot(block_rows, up_matrix, preferred_element_type=jnp.float32)).astype(
        jnp.bfloat16
    )
    return jnp.dot(hidden, down_matrix, preferred_element_type=jnp.float32)


def slots_of(ids, slot_size):
    count = ids.shape[0]
    row = lax.broadcasted_iota(jnp.int32, (count, count), 0)
    col = lax.broadcasted_iota(jnp.int32, (count, count), 1)
    before = (ids[:, None] == ids[None, :]) & (col < row)
    return ids * slot_size + jnp.sum(before.astype(jnp.int32), axis=1)


def counts_of(ids, half):
    experts = lax.broadcasted_iota(jnp.int32, (half, ids.shape[0]), 0)
    return jnp.sum((experts == ids[None, :]).astype(jnp.int32), axis=1)


def spread(rows, slots, slot_total):
    place = lax.broadcasted_iota(jnp.int32, (slot_total, rows.shape[0]), 0) == slots[None, :]
    return jnp.dot(place.astype(jnp.bfloat16), rows, preferred_element_type=jnp.float32).astype(
        jnp.bfloat16
    )


def pick(slot_rows, slots):
    place = (
        lax.broadcasted_iota(jnp.int32, (slots.shape[0], slot_rows.shape[0]), 1) == slots[:, None]
    )
    return jnp.dot(place.astype(jnp.bfloat16), slot_rows, preferred_element_type=jnp.float32)


def shards(
    query_features,
    query_job_label,
    selected_specialists,
    whole_number_mixing_factors,
    copy_room_sizes,
    first_layer_matrix,
    second_layer_matrix,
):
    experts = copy_room_sizes.shape[0]
    half = experts // 2
    row_count, width = query_features.shape
    copies = half // SHARED
    slot_size = 4 * row_count // experts
    slot_total = half * slot_size
    up_matrix = first_layer_matrix[0]
    down_matrix = second_layer_matrix[0]
    me = lax.axis_index("expert")
    upper = me >= half
    swap = [(i, (i + half) % experts) for i in range(experts)]
    halves = [list(range(half)), list(range(half, experts))]

    by_permutes = half <= 8 and half & (half - 1) == 0
    place = me % half

    def relative(ids):
        return ids ^ place if by_permutes else ids

    def exchange(array):
        return lax.all_to_all(
            array, "expert", split_axis=0, concat_axis=0, axis_index_groups=halves, tiled=True
        )

    def exchange_rows(rows):
        if not by_permutes:
            return exchange(rows.reshape(half, slot_size, width)).reshape(slot_total, width)
        blocks = {0: rows[:slot_size]}
        for b in range(half - 1, 0, -1):
            pairs = [(i, i ^ b) for i in range(experts)]
            blocks[b] = lax.ppermute(rows[b * slot_size : (b + 1) * slot_size], "expert", pairs)
        return jnp.concatenate([blocks[b] for b in range(half)], axis=0)

    def by_sender(base):
        if not by_permutes:
            return base
        index = jnp.arange(half, dtype=jnp.int32)
        sender = index ^ place
        return jnp.sum(jnp.where(sender[:, None] == index[None, :], base[None, :], 0), axis=1)

    task_id = query_job_label * copies + selected_specialists[:, 0] - SHARED
    row_local = jnp.arange(row_count, dtype=jnp.int32)
    shared_id = selected_specialists[:, 1] * copies + row_local % copies
    near_id = jnp.where(upper, task_id, shared_id)
    far_id = jnp.where(upper, shared_id, task_id)

    guest_rows = lax.ppermute(query_features, "expert", swap)
    guest_id = lax.ppermute(far_id, "expert", swap)

    near_slots = slots_of(relative(near_id), slot_size)
    near_in = exchange_rows(spread(query_features, near_slots, slot_total))
    guest_slots = slots_of(relative(guest_id), slot_size)
    counts = exchange(
        jnp.stack([counts_of(near_id, half), counts_of(guest_id, half)], axis=1)
    )
    near_in, guest_spread = lax.optimization_barrier(
        (near_in, spread(guest_rows, guest_slots, slot_total))
    )
    guest_in = exchange_rows(guest_spread)

    earlier = (
        lax.broadcasted_iota(jnp.int32, (half, half), 1)
        < lax.broadcasted_iota(jnp.int32, (half, half), 0)
    ).astype(jnp.int32)
    near_base = jnp.sum(earlier * counts[None, :, 0], axis=1) + jnp.where(
        upper, jnp.sum(counts[:, 1]), 0
    )
    guest_base = jnp.sum(earlier * counts[None, :, 1], axis=1) + jnp.where(
        upper, 0, jnp.sum(counts[:, 0])
    )
    room = copy_room_sizes[me]
    slot_local = jnp.arange(slot_size, dtype=jnp.int32)

    def serve(arrived, base):
        keep = (by_sender(base)[:, None] + slot_local[None, :] < room).reshape(-1, 1)
        result = expert_mlp(arrived, up_matrix, down_matrix)
        kept = jnp.where(keep, result, 0.0).astype(jnp.bfloat16)
        return exchange_rows(kept)

    guest_out = pick(serve(guest_in, guest_base), guest_slots).astype(jnp.bfloat16)
    far_out = lax.ppermute(guest_out, "expert", swap).astype(jnp.float32)
    near_out = pick(serve(near_in, near_base), near_slots)

    gate_float = whole_number_mixing_factors.astype(jnp.float32)
    gate_share = gate_float / jnp.sum(gate_float, axis=1, keepdims=True)
    near_share = jnp.where(upper, gate_share[:, 0], gate_share[:, 1])
    far_share = jnp.where(upper, gate_share[:, 1], gate_share[:, 0])
    return (near_share[:, None] * near_out + far_share[:, None] * far_out).astype(jnp.bfloat16)


def solution(mesh):
    in_specs = (
        P(("groups", "expert"), None),
        P(("groups", "expert")),
        P(("groups", "expert"), None),
        P(("groups", "expert"), None),
        P(),
        P("expert", None, None),
        P("expert", None, None),
    )
    out_specs = P(("groups", "expert"), None)
    return jax.shard_map(shards, mesh=mesh, in_specs=in_specs, out_specs=out_specs, check_vma=False)
```

```python
import jax
import jax.numpy as jnp
from jax import lax
from jax.sharding import PartitionSpec as P


SHARED = 8
EXTRA = 8


def expert_mlp(block_rows, up_matrix, down_matrix):
    hidden = jax.nn.gelu(jnp.dot(block_rows, up_matrix, preferred_element_type=jnp.float32)).astype(
        jnp.bfloat16
    )
    return jnp.dot(hidden, down_matrix, preferred_element_type=jnp.float32)


def slots_of(ids, slot_size):
    count = ids.shape[0]
    row = lax.broadcasted_iota(jnp.int32, (count, count), 0)
    col = lax.broadcasted_iota(jnp.int32, (count, count), 1)
    before = (ids[:, None] == ids[None, :]) & (col < row)
    return ids * slot_size + jnp.sum(before.astype(jnp.int32), axis=1)


def counts_of(ids, half):
    experts = lax.broadcasted_iota(jnp.int32, (half, ids.shape[0]), 0)
    return jnp.sum((experts == ids[None, :]).astype(jnp.int32), axis=1)


def spread(rows, slots, slot_total):
    place = lax.broadcasted_iota(jnp.int32, (slot_total, rows.shape[0]), 0) == slots[None, :]
    return jnp.dot(place.astype(jnp.bfloat16), rows, preferred_element_type=jnp.float32).astype(
        jnp.bfloat16
    )


def pick(slot_rows, slots):
    place = (
        lax.broadcasted_iota(jnp.int32, (slots.shape[0], slot_rows.shape[0]), 1) == slots[:, None]
    )
    return jnp.dot(place.astype(jnp.bfloat16), slot_rows, preferred_element_type=jnp.float32)


def shards(
    query_features,
    query_job_label,
    selected_specialists,
    whole_number_mixing_factors,
    copy_room_sizes,
    first_layer_matrix,
    second_layer_matrix,
):
    experts = copy_room_sizes.shape[0]
    half = experts // 2
    row_count, width = query_features.shape
    copies = half // SHARED
    slot_size = 4 * row_count // experts
    slot_total = half * slot_size
    up_matrix = first_layer_matrix[0]
    down_matrix = second_layer_matrix[0]
    me = lax.axis_index("expert")
    upper = me >= half
    swap = [(i, (i + half) % experts) for i in range(experts)]
    halves = [list(range(half)), list(range(half, experts))]

    def exchange(array):
        return lax.all_to_all(
            array, "expert", split_axis=0, concat_axis=0, axis_index_groups=halves, tiled=True
        )

    task_id = query_job_label * copies + selected_specialists[:, 0] - SHARED
    row_local = jnp.arange(row_count, dtype=jnp.int32)
    shared_id = selected_specialists[:, 1] * copies + row_local % copies
    near_id = jnp.where(upper, task_id, shared_id)
    far_id = jnp.where(upper, shared_id, task_id)

    guest_rows = lax.ppermute(query_features, "expert", swap)
    guest_id = lax.ppermute(far_id, "expert", swap)

    block = slot_size + EXTRA
    near_slots = slots_of(near_id, block)
    notes = jnp.stack([counts_of(near_id, half), counts_of(guest_id, half)], axis=1)
    fill = jnp.pad(notes, ((0, 0), (slot_size, EXTRA - 2))).reshape(-1, 1).astype(jnp.float32)
    place = lax.broadcasted_iota(jnp.int32, (half * block, row_count), 0) == near_slots[None, :]
    near_out_blocks = (
        jnp.dot(place.astype(jnp.bfloat16), query_features, preferred_element_type=jnp.float32)
        + fill
    ).astype(jnp.bfloat16)
    near_blocks = exchange(near_out_blocks.reshape(half, block, width))
    near_blocks, guest_rows = lax.optimization_barrier((near_blocks, guest_rows))

    guest_slots = slots_of(guest_id, slot_size)
    guest_spread = spread(guest_rows, guest_slots, slot_total)
    near_blocks, guest_spread = lax.optimization_barrier((near_blocks, guest_spread))
    guest_in = exchange(guest_spread.reshape(half, slot_size, width))
    near_in = near_blocks[:, :slot_size]
    counts = jnp.max(near_blocks[:, slot_size:, :128].astype(jnp.float32), axis=2).astype(jnp.int32)

    earlier = (
        lax.broadcasted_iota(jnp.int32, (half, half), 1)
        < lax.broadcasted_iota(jnp.int32, (half, half), 0)
    ).astype(jnp.int32)
    near_base = jnp.sum(earlier * counts[None, :, 0], axis=1) + jnp.where(
        upper, jnp.sum(counts[:, 1]), 0
    )
    guest_base = jnp.sum(earlier * counts[None, :, 1], axis=1) + jnp.where(
        upper, 0, jnp.sum(counts[:, 0])
    )
    room = copy_room_sizes[me]
    slot_local = jnp.arange(slot_size, dtype=jnp.int32)

    def serve(arrived, base):
        keep = (base[:, None] + slot_local[None, :] < room).reshape(-1, 1)
        result = expert_mlp(arrived.reshape(slot_total, width), up_matrix, down_matrix)
        return jnp.where(keep, result, 0.0).astype(jnp.bfloat16)

    near_served = serve(near_in, near_base)
    guest_served = serve(guest_in, guest_base)
    guest_back = exchange(guest_served.reshape(half, slot_size, width))
    guest_out = pick(guest_back.reshape(slot_total, width), guest_slots).astype(jnp.bfloat16)
    near_served, guest_out = lax.optimization_barrier((near_served, guest_out))
    far_out = lax.ppermute(guest_out, "expert", swap).astype(jnp.float32)
    near_back = exchange(near_served.reshape(half, slot_size, width))
    near_out = pick(near_back.reshape(slot_total, width), near_slots // block * slot_size + near_slots % block)

    gate_float = whole_number_mixing_factors.astype(jnp.float32)
    gate_share = gate_float / jnp.sum(gate_float, axis=1, keepdims=True)
    near_share = jnp.where(upper, gate_share[:, 0], gate_share[:, 1])
    far_share = jnp.where(upper, gate_share[:, 1], gate_share[:, 0])
    return (near_share[:, None] * near_out + far_share[:, None] * far_out).astype(jnp.bfloat16)


def solution(mesh):
    in_specs = (
        P(("groups", "expert"), None),
        P(("groups", "expert")),
        P(("groups", "expert"), None),
        P(("groups", "expert"), None),
        P(),
        P("expert", None, None),
        P("expert", None, None),
    )
    out_specs = P(("groups", "expert"), None)

    return jax.shard_map(shards, mesh=mesh, in_specs=in_specs, out_specs=out_specs, check_vma=False)
```

```python
import jax
import jax.numpy as jnp
from jax import lax
from jax.sharding import PartitionSpec as P


SHARED = 8
EXTRA = 8


def expert_mlp(block_rows, up_matrix, down_matrix):
    hidden = jax.nn.gelu(jnp.dot(block_rows, up_matrix, preferred_element_type=jnp.float32)).astype(
        jnp.bfloat16
    )
    return jnp.dot(hidden, down_matrix, preferred_element_type=jnp.float32)


def slots_of(ids, slot_size):
    count = ids.shape[0]
    row = lax.broadcasted_iota(jnp.int32, (count, count), 0)
    col = lax.broadcasted_iota(jnp.int32, (count, count), 1)
    before = (ids[:, None] == ids[None, :]) & (col < row)
    return ids * slot_size + jnp.sum(before.astype(jnp.int32), axis=1)


def counts_of(ids, half):
    experts = lax.broadcasted_iota(jnp.int32, (half, ids.shape[0]), 0)
    return jnp.sum((experts == ids[None, :]).astype(jnp.int32), axis=1)


def spread(rows, slots, slot_total):
    place = lax.broadcasted_iota(jnp.int32, (slot_total, rows.shape[0]), 0) == slots[None, :]
    return jnp.dot(place.astype(jnp.bfloat16), rows, preferred_element_type=jnp.float32).astype(
        jnp.bfloat16
    )


def pick(slot_rows, slots):
    place = (
        lax.broadcasted_iota(jnp.int32, (slots.shape[0], slot_rows.shape[0]), 1) == slots[:, None]
    )
    return jnp.dot(place.astype(jnp.bfloat16), slot_rows, preferred_element_type=jnp.float32)


def shards(
    query_features,
    query_job_label,
    selected_specialists,
    whole_number_mixing_factors,
    copy_room_sizes,
    first_layer_matrix,
    second_layer_matrix,
):
    experts = copy_room_sizes.shape[0]
    half = experts // 2
    row_count, width = query_features.shape
    copies = half // SHARED
    slot_size = 4 * row_count // experts
    slot_total = half * slot_size
    up_matrix = first_layer_matrix[0]
    down_matrix = second_layer_matrix[0]
    me = lax.axis_index("expert")
    upper = me >= half
    swap = [(i, (i + half) % experts) for i in range(experts)]
    halves = [list(range(half)), list(range(half, experts))]

    def exchange(array):
        return lax.all_to_all(
            array, "expert", split_axis=0, concat_axis=0, axis_index_groups=halves, tiled=True
        )

    task_id = query_job_label * copies + selected_specialists[:, 0] - SHARED
    row_local = jnp.arange(row_count, dtype=jnp.int32)
    shared_id = selected_specialists[:, 1] * copies + row_local % copies
    near_id = jnp.where(upper, task_id, shared_id)
    far_id = jnp.where(upper, shared_id, task_id)

    guest_rows = lax.ppermute(query_features, "expert", swap)
    guest_id = lax.ppermute(far_id, "expert", swap)

    block = slot_size + EXTRA
    near_slots = slots_of(near_id, block)
    notes = jnp.stack([counts_of(near_id, half), counts_of(guest_id, half)], axis=1)
    fill = jnp.pad(notes, ((0, 0), (slot_size, EXTRA - 2))).reshape(-1, 1).astype(jnp.float32)
    place = lax.broadcasted_iota(jnp.int32, (half * block, row_count), 0) == near_slots[None, :]
    near_out_blocks = (
        jnp.dot(place.astype(jnp.bfloat16), query_features, preferred_element_type=jnp.float32)
        + fill
    ).astype(jnp.bfloat16)
    near_blocks = exchange(near_out_blocks.reshape(half, block, width))
    near_blocks, guest_rows = lax.optimization_barrier((near_blocks, guest_rows))

    guest_slots = slots_of(guest_id, slot_size)
    guest_spread = spread(guest_rows, guest_slots, slot_total)
    near_blocks, guest_spread = lax.optimization_barrier((near_blocks, guest_spread))
    guest_in = exchange(guest_spread.reshape(half, slot_size, width))
    near_in = near_blocks[:, :slot_size]
    counts = jnp.max(near_blocks[:, slot_size:, :128].astype(jnp.float32), axis=2).astype(jnp.int32)

    earlier = (
        lax.broadcasted_iota(jnp.int32, (half, half), 1)
        < lax.broadcasted_iota(jnp.int32, (half, half), 0)
    ).astype(jnp.int32)
    near_base = jnp.sum(earlier * counts[None, :, 0], axis=1) + jnp.where(
        upper, jnp.sum(counts[:, 1]), 0
    )
    guest_base = jnp.sum(earlier * counts[None, :, 1], axis=1) + jnp.where(
        upper, 0, jnp.sum(counts[:, 0])
    )
    room = copy_room_sizes[me]
    slot_local = jnp.arange(slot_size, dtype=jnp.int32)

    def serve(arrived, base):
        keep = (base[:, None] + slot_local[None, :] < room).reshape(-1, 1)
        result = expert_mlp(arrived.reshape(slot_total, width), up_matrix, down_matrix)
        return jnp.where(keep, result, 0.0).astype(jnp.bfloat16)

    near_served = serve(near_in, near_base)
    sent = jnp.concatenate([near_served, near_served], axis=0)
    sent, guest_in = lax.optimization_barrier((sent, guest_in))
    guest_served = serve(guest_in, guest_base)
    start = jnp.where(upper, 0, slot_total)
    sent = lax.dynamic_update_slice(sent, guest_served, (start, jnp.zeros_like(start)))
    returned = lax.all_to_all(
        sent.reshape(experts, slot_size, width), "expert", split_axis=0, concat_axis=0, tiled=True
    ).reshape(experts * slot_size, width)

    gate_float = whole_number_mixing_factors.astype(jnp.float32)
    gate_share = gate_float / jnp.sum(gate_float, axis=1, keepdims=True)
    task_out = pick(returned, slots_of(half + task_id, slot_size))
    shared_out = pick(returned, slots_of(shared_id, slot_size))
    return (gate_share[:, :1] * task_out + gate_share[:, 1:] * shared_out).astype(jnp.bfloat16)


def solution(mesh):
    in_specs = (
        P(("groups", "expert"), None),
        P(("groups", "expert")),
        P(("groups", "expert"), None),
        P(("groups", "expert"), None),
        P(),
        P("expert", None, None),
        P("expert", None, None),
    )
    out_specs = P(("groups", "expert"), None)

    return jax.shard_map(shards, mesh=mesh, in_specs=in_specs, out_specs=out_specs, check_vma=False)
```

```python
import jax
import jax.numpy as jnp
from jax import lax
from jax.sharding import PartitionSpec as P

SHARED = 8
EMPTY = 64.0


def expert_mlp(block_rows, up_matrix, down_matrix):
    hidden = jax.nn.gelu(jnp.dot(block_rows, up_matrix, preferred_element_type=jnp.float32)).astype(
        jnp.bfloat16
    )
    return jnp.dot(hidden, down_matrix, preferred_element_type=jnp.float32)


def slots_of(ids, slot_size):
    count = ids.shape[0]
    row = lax.broadcasted_iota(jnp.int32, (count, count), 0)
    col = lax.broadcasted_iota(jnp.int32, (count, count), 1)
    before = (ids[:, None] == ids[None, :]) & (col < row)
    return ids * slot_size + jnp.sum(before.astype(jnp.int32), axis=1)


def pick(slot_rows, slots):
    place = (
        lax.broadcasted_iota(jnp.int32, (slots.shape[0], slot_rows.shape[0]), 1) == slots[:, None]
    )
    return jnp.dot(place.astype(jnp.bfloat16), slot_rows, preferred_element_type=jnp.float32)


def shards(
    query_features,
    query_job_label,
    selected_specialists,
    whole_number_mixing_factors,
    copy_room_sizes,
    first_layer_matrix,
    second_layer_matrix,
):
    experts = copy_room_sizes.shape[0]
    half = experts // 2
    row_count, width = query_features.shape
    copies = half // SHARED
    slot_size = 4 * row_count // experts
    slot_total = experts * slot_size
    me = lax.axis_index("expert")

    task_id = half + query_job_label * copies + selected_specialists[:, 0] - SHARED
    row_local = jnp.arange(row_count, dtype=jnp.int32)
    shared_id = selected_specialists[:, 1] * copies + row_local % copies
    task_slots = slots_of(task_id, slot_size)
    shared_slots = slots_of(shared_id, slot_size)

    slot = lax.broadcasted_iota(jnp.int32, (slot_total, row_count), 0)
    place = (slot == task_slots[None, :]) | (slot == shared_slots[None, :])
    fill = EMPTY - EMPTY * jnp.sum(place.astype(jnp.float32), axis=1, keepdims=True)
    placed = jnp.dot(place.astype(jnp.bfloat16), query_features, preferred_element_type=jnp.float32)
    sent = (placed + fill).astype(jnp.bfloat16)
    arrived = lax.all_to_all(
        sent.reshape(experts, slot_size, width), "expert", split_axis=0, concat_axis=0, tiled=True
    )

    level = jnp.max(arrived[:, :, :128].astype(jnp.float32), axis=2)
    counts = jnp.sum((level < EMPTY / 2).astype(jnp.int32), axis=1)
    earlier = (
        lax.broadcasted_iota(jnp.int32, (experts, experts), 1)
        < lax.broadcasted_iota(jnp.int32, (experts, experts), 0)
    ).astype(jnp.int32)
    base = jnp.sum(earlier * counts[None, :], axis=1)
    slot_local = jnp.arange(slot_size, dtype=jnp.int32)[None, :]
    keep = (slot_local < counts[:, None]) & (base[:, None] + slot_local < copy_room_sizes[me])
    result = expert_mlp(
        arrived.reshape(slot_total, width), first_layer_matrix[0], second_layer_matrix[0]
    )
    kept = jnp.where(keep.reshape(-1, 1), result, 0.0).astype(jnp.bfloat16)
    returned = lax.all_to_all(
        kept.reshape(experts, slot_size, width), "expert", split_axis=0, concat_axis=0, tiled=True
    ).reshape(slot_total, width)

    gate_float = whole_number_mixing_factors.astype(jnp.float32)
    gate_share = gate_float / jnp.sum(gate_float, axis=1, keepdims=True)
    task_out = pick(returned, task_slots)
    shared_out = pick(returned, shared_slots)
    return (gate_share[:, :1] * task_out + gate_share[:, 1:] * shared_out).astype(jnp.bfloat16)


def solution(mesh):
    in_specs = (
        P(("groups", "expert"), None),
        P(("groups", "expert")),
        P(("groups", "expert"), None),
        P(("groups", "expert"), None),
        P(),
        P("expert", None, None),
        P("expert", None, None),
    )
    out_specs = P(("groups", "expert"), None)
    return jax.shard_map(shards, mesh=mesh, in_specs=in_specs, out_specs=out_specs, check_vma=False)
```
